32 devices in a mesh: dp: 16 (over z, y, core), mp: 2 (over x).
Axes of the slice: x: 2, y: 2, z: 4, core: 2. Of those that a mesh axis runs over, the one named last changes fastest.
Arguments:
- activations: bfloat16 [8192, 1792], P('dp', 'mp'), may hold values from -6 to 6
- projection: bfloat16 [1792, 9216], P('mp', 'dp'), may hold values from -0.125 to 0.125
Outputs:
- projected: bfloat16 [8192, 9216], P('dp', 'mp')
The draws below stay inside these ranges and needn't reach their ends.
All inputs are finite; a program needn't handle non-finite values.
Results may differ from the reference program's by a relative error of at most 0.001.
Values may be sent and summed in bfloat16 or wider, within the bound.
A program may use at most 128 MiB of HBM per device.

```python
import jax
import jax.numpy as jnp
from jax import lax

D_MP = 896
F = 9216
TOK_DEV = 512
D = 1792
TOKENS = 8192
N_DP = 16
N_MP = 2


def levels(key, dims, pieces, smallest, high):
    factor_of, own = 1.0, jax.random.fold_in(key, 6)
    for position, blocks in pieces:
        draws = jnp.exp(jax.random.uniform(jax.random.fold_in(own, position), (blocks,), jnp.float32, smallest / len(pieces), high / len(pieces)))
        factor_of = factor_of * jnp.repeat(draws, dims[position] // blocks).reshape([-1 if axis == position else 1 for axis in range(len(dims))])
    return factor_of


def normal_values(stream_key, dims, scale, limit, split=(), held_as=jnp.bfloat16):
    values = scale * jax.random.normal(stream_key, dims, jnp.float32)
    if split:
        values = values * levels(stream_key, dims, split, -0.22, 0.18)
    return jnp.clip(values, -limit, limit).astype(held_as)


def setup_inputs(seed: int = 0) -> dict:
    streams_of = jax.random.split(jax.random.key(seed), 3)
    return {
        "activations": normal_values(streams_of[0], (TOKENS, D), 1.0, 6.0, ((0, 16), (1, 2))),
        "projection": normal_values(streams_of[1], (D, F), D ** -0.5, 0.125, ((0, 2), (1, 16))),
    }


def reference(activations, projection):
    block_rows = TOK_DEV
    blocks = activations.reshape(N_DP, block_rows, D_MP * N_MP)

    def one_block(rows):
        return jnp.dot(rows, projection, preferred_element_type=jnp.float32).astype(jnp.bfloat16)

    result = lax.map(one_block, blocks)
    return result.reshape(N_DP * block_rows, F)
```

```python
import functools

import jax
import jax.numpy as jnp
from jax import lax
from jax.experimental import pallas as pl
from jax.experimental.pallas import tpu as pltpu
from jax.sharding import PartitionSpec as P

MESH = pl.DeviceIdType.MESH
LANES = 128
ACT_PIECES = 4
MM_LAG = 4


def general(activations, projection):
    wide_rows = lax.all_gather(activations, "mp", axis=1, tiled=True)
    local_cols = lax.all_to_all(projection, "mp", split_axis=1, concat_axis=0, tiled=True)
    finished = jnp.dot(
        wide_rows,
        lax.all_gather(local_cols, "dp", axis=1, tiled=True),
        preferred_element_type=jnp.float32,
    )
    finished = finished.astype(jnp.bfloat16)
    tok_rows = finished.shape[0]
    blocks = lax.axis_size("dp")
    share = local_cols.shape[1]
    sectioned = finished.reshape(tok_rows, blocks, 1, share)
    placed = lax.all_to_all(sectioned, "mp", split_axis=1, concat_axis=2, tiled=True)
    return placed.reshape(tok_rows, placed.shape[1] * placed.shape[2] * share)


def kernel(nz, a_ref, w_ref, o_ref, big, acts, stage, outs, send_sem, recv_sem,
           act_send, act_recv, loc_sem, stage_sem, out_sem):
    d, x = lax.axis_index("dp"), lax.axis_index("mp")
    z, y, c = d // 4, (d // 2) % 2, d % 2
    half = nz // 2
    pair = big.shape[2]
    depth = w_ref.shape[0]
    part = depth // 2
    steps = pair // LANES
    rows = a_ref.shape[0]
    lane = x * 2 + c
    core_dev = (d + 1 - 2 * c, x)
    y_dev = (d + 2 - 4 * y, x)
    x_dev = (d, 1 - x)
    up_dev = (lax.rem(d + 4, 4 * nz), x)
    down_dev = (lax.rem(d + 4 * nz - 4, 4 * nz), x)
    can_up, can_down = z < nz - 1, z > 0

    own_act = pltpu.make_async_copy(
        a_ref, acts.at[:, pl.ds(pl.multiple_of(x * depth, LANES), depth)], loc_sem.at[0])
    own_act.start()
    mine_rows = pltpu.make_async_copy(
        w_ref.at[pl.ds(pl.multiple_of(c * part, 16), part), :], stage.at[c], loc_sem.at[1])
    mine_rows.start()

    barrier = pltpu.get_barrier_semaphore()
    for dev in (core_dev, y_dev, x_dev):
        pl.semaphore_signal(barrier, inc=1, device_id=dev, device_id_type=MESH)

    @pl.when(can_up)
    def _():
        pl.semaphore_signal(barrier, inc=1, device_id=up_dev, device_id_type=MESH)

    @pl.when(can_down)
    def _():
        pl.semaphore_signal(barrier, inc=1, device_id=down_dev, device_id_type=MESH)

    pl.semaphore_wait(barrier, 3 + can_up.astype(jnp.int32) + can_down.astype(jnp.int32))

    swap = pltpu.make_async_remote_copy(
        src_ref=w_ref.at[pl.ds(pl.multiple_of((1 - c) * part, 16), part), :],
        dst_ref=stage.at[c], send_sem=stage_sem.at[0], recv_sem=stage_sem.at[1],
        device_id=core_dev, device_id_type=MESH)
    swap.start()
    mine_rows.wait()
    swap.wait()
    big[z * 2 + y, pl.ds(pl.multiple_of(lane * part, 16), part), :] = jnp.concatenate(
        [stage[0], stage[1]], axis=1)

    def copy(kind, zz, yy, q, s, dev):
        piece = big.at[zz * 2 + yy, pl.ds(pl.multiple_of(q * part, 16), part),
                       pl.ds(pl.multiple_of(s * LANES, LANES), LANES)]
        return pltpu.make_async_remote_copy(
            src_ref=piece, dst_ref=piece, send_sem=send_sem.at[kind, zz, s],
            recv_sem=recv_sem.at[zz, yy, q, s], device_id=dev, device_id_type=MESH)

    def z_stage(s, act, arrive):
        def lane_piece(zz, up, down):
            @pl.when(up)
            def _():
                act(copy(0, zz, y, lane, s, up_dev))

            @pl.when(down)
            def _():
                act(copy(1, zz, y, lane, s, down_dev))

            @pl.when(zz // half == x)
            def _():
                act(copy(2, zz, y, lane, s, y_dev))
                act(copy(3, zz, y, lane, s, core_dev))

            @pl.when(zz // half != x)
            def _():
                act(copy(2, zz, y, lane, s, x_dev))

        lane_piece(z, can_up, can_down)
        for dist in range(1, nz):
            @pl.when(z >= dist)
            def _():
                arrive(z - dist, y, lane, s)
                lane_piece(z - dist, can_up, z < 0)

            @pl.when(z + dist < nz)
            def _():
                arrive(z + dist, y, lane, s)
                lane_piece(z + dist, z < 0, can_down)

    def x_stage(s, act, arrive):
        for h in range(half):
            zz, q = x * half + h, (1 - x) * 2 + c
            arrive(zz, y, q, s)
            act(copy(4, zz, y, q, s, y_dev))
            act(copy(5, zz, y, q, s, core_dev))

    def y_stage(s, act, arrive):
        for h in range(half):
            for xx in range(2):
                zz, q = x * half + h, xx * 2 + c
                arrive(zz, 1 - y, q, s)
                act(copy(6 + xx, zz, 1 - y, q, s, core_dev))

    def core_stage(s, arrive):
        for h in range(half):
            for yy in range(2):
                for xx in range(2):
                    arrive(x * half + h, yy, xx * 2 + 1 - c, s)

    def start(cp):
        cp.start()

    def drain(cp):
        cp.wait_send()

    def arrive(zz, yy, q, s):
        copy(0, zz, yy, q, s, core_dev).wait_recv()

    def no_arrive(zz, yy, q, s):
        pass

    act_rows = rows // ACT_PIECES

    def act_copy(k):
        piece = pl.ds(pl.multiple_of(k * act_rows, 16), act_rows)
        return pltpu.make_async_remote_copy(
            src_ref=a_ref.at[piece, :],
            dst_ref=acts.at[piece, pl.ds(pl.multiple_of(x * depth, LANES), depth)],
            send_sem=act_send.at[k], recv_sem=act_recv.at[k],
            device_id=x_dev, device_id_type=MESH)

    def act_in(k):
        piece = pl.ds(pl.multiple_of(k * act_rows, 16), act_rows)
        return pltpu.make_async_remote_copy(
            src_ref=a_ref.at[piece, :],
            dst_ref=acts.at[piece, pl.ds(pl.multiple_of((1 - x) * depth, LANES), depth)],
            send_sem=act_send.at[k], recv_sem=act_recv.at[k],
            device_id=x_dev, device_id_type=MESH)

    def out_copy(b, s):
        cols = pl.ds(pl.multiple_of(b * pair + s * LANES, LANES), LANES)
        return pltpu.make_async_copy(outs.at[:, cols], o_ref.at[:, cols], out_sem.at[b, s])

    def multiply(s):
        cols = pl.ds(pl.multiple_of(s * LANES, LANES), LANES)
        for b in range(0, 2 * half, 2):
            base = x * 2 * half + b
            rhs = jnp.concatenate([big[base, :, cols], big[base + 1, :, cols]], axis=1)
            res = jnp.dot(acts[...], rhs, preferred_element_type=jnp.float32).astype(jnp.bfloat16)
            for k in range(2):
                at = pl.ds(pl.multiple_of((b + k) * pair + s * LANES, LANES), LANES)
                outs[:, at] = res[:, k * LANES:(k + 1) * LANES]
                out_copy(b + k, s).start()

    def within(s):
        return jnp.logical_and(s >= 0, s < steps)

    def step(i, carry):
        @pl.when(within(i))
        def _():
            z_stage(i, start, arrive)

        @pl.when(i < ACT_PIECES)
        def _():
            act_copy(i).start()

        @pl.when(within(i - 1))
        def _():
            x_stage(i - 1, start, arrive)

        @pl.when(within(i - 2))
        def _():
            y_stage(i - 2, start, arrive)

        @pl.when(i == MM_LAG)
        def _():
            own_act.wait()
            for k in range(ACT_PIECES):
                act_in(k).wait_recv()

        @pl.when(within(i - MM_LAG))
        def _():
            core_stage(i - MM_LAG, arrive)
            multiply(i - MM_LAG)

        return carry

    lax.fori_loop(0, steps + MM_LAG, step, 0)

    def finish(s, carry):
        z_stage(s, drain, no_arrive)
        x_stage(s, drain, no_arrive)
        y_stage(s, drain, no_arrive)
        for b in range(2 * half):
            out_copy(b, s).wait()
        return carry

    lax.fori_loop(0, steps, finish, 0)
    for k in range(ACT_PIECES):
        act_copy(k).wait_send()


def gathered(nz, activations, projection):
    rows, depth = activations.shape
    width = projection.shape[1]
    pair, steps, half = 2 * width, 2 * width // LANES, nz // 2
    columns = nz * 2 * pair // 2
    dma = pltpu.SemaphoreType.DMA
    return pl.pallas_call(
        functools.partial(kernel, nz),
        out_shape=jax.ShapeDtypeStruct((rows, columns), jnp.bfloat16),
        in_specs=[pl.BlockSpec(memory_space=pl.ANY)] * 2,
        out_specs=pl.BlockSpec(memory_space=pl.ANY),
        scratch_shapes=[
            pltpu.VMEM((nz * 2, 2 * depth, pair), jnp.bfloat16),
            pltpu.VMEM((rows, 2 * depth), jnp.bfloat16),
            pltpu.VMEM((2, depth // 2, width), jnp.bfloat16),
            pltpu.VMEM((rows, columns), jnp.bfloat16),
            dma((8, nz, steps)),
            dma((nz, 2, 4, steps)),
            dma((ACT_PIECES,)),
            dma((ACT_PIECES,)),
            dma((2,)),
            dma((2,)),
            dma((2 * half, steps)),
        ],
        compiler_params=pltpu.CompilerParams(
            collective_id=0, has_side_effects=True, vmem_limit_bytes=60 * 2**20),
    )(activations, projection)


def solution(mesh):
    n_dp, n_mp = mesh.shape["dp"], mesh.shape["mp"]

    def shards(activations, projection):
        rows, depth = activations.shape
        width = projection.shape[1]
        nz = n_dp // 4
        fits = (
            n_mp == 2 and n_dp % 8 == 0 and (2 * width) % LANES == 0
            and depth % LANES == 0 and (depth // 2) % 16 == 0 and rows % (16 * ACT_PIECES) == 0
            and nz * 2 * 2 * depth * 2 * width * 2 <= 36 * 2**20 and nz <= 4
        )
        if fits:
            return gathered(nz, activations, projection)
        return general(activations, projection)

    placed = (P("dp", "mp"), P("mp", "dp"))
    return jax.shard_map(
        shards, mesh=mesh, in_specs=placed, out_specs=P("dp", "mp"), check_vma=False
    )
```

```python
import functools

import jax
import jax.numpy as jnp
from jax import lax
from jax.experimental import pallas as pl
from jax.experimental.pallas import tpu as pltpu
from jax.sharding import PartitionSpec as P

MESH = pl.DeviceIdType.MESH
LANES = 128
ACT_PIECES = 4
UNIT = 64
DUP = 2
SKEW = 1


def general(activations, projection):
    wide_rows = lax.all_gather(activations, "mp", axis=1, tiled=True)
    local_cols = lax.all_to_all(projection, "mp", split_axis=1, concat_axis=0, tiled=True)
    finished = jnp.dot(
        wide_rows,
        lax.all_gather(local_cols, "dp", axis=1, tiled=True),
        preferred_element_type=jnp.float32,
    )
    finished = finished.astype(jnp.bfloat16)
    tok_rows = finished.shape[0]
    blocks = lax.axis_size("dp")
    share = local_cols.shape[1]
    sectioned = finished.reshape(tok_rows, blocks, 1, share)
    placed = lax.all_to_all(sectioned, "mp", split_axis=1, concat_axis=2, tiled=True)
    return placed.reshape(tok_rows, placed.shape[1] * placed.shape[2] * share)


def kernel(nz, a_ref, w_ref, o_ref, big, acts, outs, send_sem, recv_sem, act_send, act_recv, loc_sem, act_loc, out_sem):
    d, x = lax.axis_index("dp"), lax.axis_index("mp")
    z, y, c = d // 4, (d // 2) % 2, d % 2
    half = nz // 2
    width, depth = w_ref.shape
    rows = a_ref.shape[0]
    steps = width // UNIT
    first_dup = steps - DUP
    per, mid = LANES // UNIT, width // LANES
    loose = (width - mid * LANES) // UNIT
    lag = SKEW * (nz + 2)
    core_dev = (d + 1 - 2 * c, x)
    y_dev = (d + 2 - 4 * y, x)
    x_dev = (d, 1 - x)
    up_dev = (lax.rem(d + 4, 4 * nz), x)
    down_dev = (lax.rem(d + 4 * nz - 4, 4 * nz), x)
    can_up, can_down, never = z < nz - 1, z > 0, z < 0

    def unit_of(cc, t):
        return lax.rem(t + (steps - loose) * (1 - cc), steps)

    def part(zz, yy, xx, cc, t):
        row = pl.multiple_of(cc * width + unit_of(cc, t) * UNIT, UNIT)
        return big.at[zz * 2 + yy, xx, pl.ds(row, UNIT), :]

    def own_copy(t):
        row = pl.multiple_of(unit_of(c, t) * UNIT, UNIT)
        return pltpu.make_async_copy(w_ref.at[pl.ds(row, UNIT), :], part(z, y, x, c, t), loc_sem.at[t])

    own_act = pltpu.make_async_copy(
        a_ref, acts.at[:, pl.ds(pl.multiple_of(x * depth, LANES), depth)], act_loc.at[0])

    def begin(t, carry):
        own_copy(t).start()
        return carry

    lax.fori_loop(0, steps, begin, 0)
    own_act.start()

    barrier = pltpu.get_barrier_semaphore()
    for dev in (core_dev, y_dev, x_dev):
        pl.semaphore_signal(barrier, inc=1, device_id=dev, device_id_type=MESH)

    @pl.when(can_up)
    def _():
        pl.semaphore_signal(barrier, inc=1, device_id=up_dev, device_id_type=MESH)

    @pl.when(can_down)
    def _():
        pl.semaphore_signal(barrier, inc=1, device_id=down_dev, device_id_type=MESH)

    pl.semaphore_wait(barrier, 3 + can_up.astype(jnp.int32) + can_down.astype(jnp.int32))

    def copy(kind, zz, yy, xx, cc, t, dev):
        piece = part(zz, yy, xx, cc, t)
        return pltpu.make_async_remote_copy(
            src_ref=piece, dst_ref=piece, send_sem=send_sem.at[kind, zz, t],
            recv_sem=recv_sem.at[zz, yy, xx * 2 + cc, t], device_id=dev, device_id_type=MESH)

    def along(kind, zz, yy, t, up, down, act):
        @pl.when(up)
        def _():
            act(copy(kind, zz, yy, x, c, t, up_dev))

        @pl.when(down)
        def _():
            act(copy(kind + 1, zz, yy, x, c, t, down_dev))

    def lane_piece(zz, t, up, down, own, act):
        along(0, zz, y, t, up, down, act)
        mine = zz // half == x
        over_y = (t < first_dup) | (t < steps if own else never)

        @pl.when(mine & over_y)
        def _():
            act(copy(2, zz, y, x, c, t, y_dev))

        @pl.when(mine)
        def _():
            act(copy(3, zz, y, x, c, t, core_dev))

        @pl.when(~mine)
        def _():
            act(copy(2, zz, y, x, c, t, x_dev))

        if own:
            @pl.when(~mine & (t >= first_dup))
            def _():
                act(copy(3, zz, y, x, c, t, y_dev))

    def twin_piece(zz, t, up, down, act):
        along(8, zz, 1 - y, t, up, down, act)

        @pl.when(zz // half == x)
        def _():
            act(copy(6, zz, 1 - y, x, c, t, core_dev))

        @pl.when(zz // half != x)
        def _():
            act(copy(6, zz, 1 - y, x, c, t, x_dev))

    def own_stage(t, act, arrive):
        lane_piece(z, t, can_up, can_down, True, act)

    def z_stage(dist, t, act, arrive):
        @pl.when(z >= dist)
        def _():
            arrive(z - dist, y, x, c, t)
            lane_piece(z - dist, t, can_up, never, False, act)

        @pl.when(z + dist < nz)
        def _():
            arrive(z + dist, y, x, c, t)
            lane_piece(z + dist, t, never, can_down, False, act)

    def twin_own_stage(t, act, arrive):
        arrive(z, 1 - y, x, c, t)
        twin_piece(z, t, can_up, can_down, act)

    def twin_z_stage(dist, t, act, arrive):
        @pl.when(z >= dist)
        def _():
            arrive(z - dist, 1 - y, x, c, t)
            twin_piece(z - dist, t, can_up, never, act)

        @pl.when(z + dist < nz)
        def _():
            arrive(z + dist, 1 - y, x, c, t)
            twin_piece(z + dist, t, never, can_down, act)

    def x_stage(h, t, act, arrive):
        zz = x * half + h
        arrive(zz, y, 1 - x, c, t)

        @pl.when(t < first_dup)
        def _():
            act(copy(4, zz, y, 1 - x, c, t, y_dev))

        act(copy(5, zz, y, 1 - x, c, t, core_dev))

    def twin_x_stage(h, t, act, arrive):
        zz = x * half + h
        arrive(zz, 1 - y, 1 - x, c, t)
        act(copy(7, zz, 1 - y, 1 - x, c, t, core_dev))

    def y_stage(h, other, t, act, arrive):
        zz = x * half + h
        xx = 1 - x if other else x
        arrive(zz, 1 - y, xx, c, t)
        act(copy(6 + other, zz, 1 - y, xx, c, t, core_dev))

    def start(cp):
        cp.start()

    def drain(cp):
        cp.wait_send()

    def arrive(zz, yy, xx, cc, t):
        copy(0, zz, yy, xx, cc, t, core_dev).wait_recv()

    def no_arrive(zz, yy, xx, cc, t):
        pass

    act_rows = rows // ACT_PIECES

    def act_copy(k, xx):
        piece = pl.ds(pl.multiple_of(k * act_rows, 16), act_rows)
        return pltpu.make_async_remote_copy(
            src_ref=a_ref.at[piece, :],
            dst_ref=acts.at[piece, pl.ds(pl.multiple_of(xx * depth, LANES), depth)],
            send_sem=act_send.at[k], recv_sem=act_recv.at[k],
            device_id=x_dev, device_id_type=MESH)

    def out_copy(b, g):
        cols = pl.ds(pl.multiple_of(b * 2 * width + g * LANES, LANES), LANES)
        return pltpu.make_async_copy(outs.at[:, cols], o_ref.at[:, cols], out_sem.at[b, g])

    def multiply(g):
        cols = pl.ds(pl.multiple_of(g * LANES, LANES), LANES)
        for b in range(0, 2 * half, 2):
            base = x * 2 * half + b
            rhs = jnp.concatenate([
                jnp.concatenate([big[base + k, 0, cols, :], big[base + k, 1, cols, :]], axis=1)
                for k in range(2)
            ], axis=0)
            res = lax.dot_general(
                acts[...], rhs, (((1,), (1,)), ((), ())), preferred_element_type=jnp.float32
            ).astype(jnp.bfloat16)
            for k in range(2):
                at = pl.ds(pl.multiple_of((b + k) * 2 * width + g * LANES, LANES), LANES)
                outs[:, at] = res[:, k * LANES:(k + 1) * LANES]
                out_copy(b + k, g).start()

    def product(t):
        for h in range(half):
            for yy in range(2):
                for xx in range(2):
                    arrive(x * half + h, yy, xx, 1 - c, t)
        past = t - (loose - 1)
        k = past // per

        def one(j, carry):
            multiply(jnp.where(past == 0, mid, jnp.where(j == 0, k - 1, mid + k)))
            return carry

        @pl.when((past >= 0) & (lax.rem(past + per, per) == 0))
        def _():
            lax.fori_loop(0, jnp.where(past == 0, 1, 2), one, 0)

    def step(i, carry):
        def at(t, stage, low=0, high=steps):
            pl.when((t >= low) & (t < high))(functools.partial(stage, t))

        def go(stage, *lead):
            return lambda t: stage(*lead, t, start, arrive)

        def own(t):
            own_copy(t).wait()
            own_stage(t, start, arrive)

        at(i, own)
        for dist in range(1, nz):
            at(i - SKEW * dist, go(z_stage, dist))
        at(i - SKEW, go(twin_own_stage), first_dup)
        for dist in range(1, nz):
            at(i - SKEW * (1 + dist), go(twin_z_stage, dist), first_dup)

        @pl.when((i >= 1) & (i <= ACT_PIECES))
        def _():
            act_copy(i - 1, x).start()

        @pl.when(i == lag)
        def _():
            own_act.wait()
            for k in range(ACT_PIECES):
                act_copy(k, 1 - x).wait_recv()

        at(i - lag, product)
        for h in range(half):
            away = jnp.abs(z - (x * half + h))
            at(i - SKEW * (away + 1), go(x_stage, h))
            at(i - SKEW * (away + 2), go(twin_x_stage, h), first_dup)
            at(i - SKEW * (away + 1), go(y_stage, h, 0), 0, first_dup)
            at(i - SKEW * (away + 2), go(y_stage, h, 1), 0, first_dup)
        return carry

    lax.fori_loop(0, steps + lag, step, 0)

    def finish(t, carry):
        own_stage(t, drain, no_arrive)
        for dist in range(1, nz):
            z_stage(dist, t, drain, no_arrive)
        for h in range(half):
            x_stage(h, t, drain, no_arrive)

        @pl.when(t < first_dup)
        def _():
            for h in range(half):
                y_stage(h, 0, t, drain, no_arrive)
                y_stage(h, 1, t, drain, no_arrive)

        @pl.when(t >= first_dup)
        def _():
            twin_own_stage(t, drain, no_arrive)
            for dist in range(1, nz):
                twin_z_stage(dist, t, drain, no_arrive)
            for h in range(half):
                twin_x_stage(h, t, drain, no_arrive)

        return carry

    lax.fori_loop(0, steps, finish, 0)
    for k in range(ACT_PIECES):
        act_copy(k, x).wait_send()
    for b in range(2 * half):
        for g in range(2 * width // LANES):
            out_copy(b, g).wait()


def gathered(nz, activations, projection):
    rows, depth = activations.shape
    width = projection.shape[1]
    steps, groups, half = width // UNIT, 2 * width // LANES, nz // 2
    columns = nz * 2 * width
    dma = pltpu.SemaphoreType.DMA
    return pl.pallas_call(
        functools.partial(kernel, nz),
        out_shape=jax.ShapeDtypeStruct((rows, columns), jnp.bfloat16),
        in_specs=[pl.BlockSpec(memory_space=pl.ANY)] * 2,
        out_specs=pl.BlockSpec(memory_space=pl.ANY),
        scratch_shapes=[
            pltpu.VMEM((nz * 2, 2, 2 * width, depth), jnp.bfloat16),
            pltpu.VMEM((rows, 2 * depth), jnp.bfloat16),
            pltpu.VMEM((rows, columns), jnp.bfloat16),
            dma((10, nz, steps)),
            dma((nz, 2, 4, steps)),
            dma((ACT_PIECES,)),
            dma((ACT_PIECES,)),
            dma((steps,)),
            dma((1,)),
            dma((2 * half, groups)),
        ],
        compiler_params=pltpu.CompilerParams(
            collective_id=0, has_side_effects=True, vmem_limit_bytes=60 * 2**20),
    )(activations, projection.T)


def solution(mesh):
    n_dp, n_mp = mesh.shape["dp"], mesh.shape["mp"]

    def shards(activations, projection):
        rows, depth = activations.shape
        width = projection.shape[1]
        nz = n_dp // 4
        fits = (
            n_mp == 2 and n_dp % 8 == 0 and width % LANES == LANES // 2
            and width > LANES and depth % LANES == 0 and rows % (16 * ACT_PIECES) == 0
            and nz * 2 * 2 * depth * 2 * width * 2 <= 36 * 2**20 and nz <= 4
        )
        if fits:
            return gathered(nz, activations, projection)
        return general(activations, projection)

    placed = (P("dp", "mp"), P("mp", "dp"))
    return jax.shard_map(
        shards, mesh=mesh, in_specs=placed, out_specs=P("dp", "mp"), check_vma=False
    )
```

```python
import functools

import jax
import jax.numpy as jnp
from jax import lax
from jax.experimental import pallas as pl
from jax.experimental.pallas import tpu as pltpu
from jax.sharding import PartitionSpec as P

MESH = pl.DeviceIdType.MESH
LANES = 128
ACT_PIECES = 4
UNIT = 64
DUP = 2
SKEW = 1


def general(activations, projection):
    wide_rows = lax.all_gather(activations, "mp", axis=1, tiled=True)
    local_cols = lax.all_to_all(projection, "mp", split_axis=1, concat_axis=0, tiled=True)
    finished = jnp.dot(
        wide_rows,
        lax.all_gather(local_cols, "dp", axis=1, tiled=True),
        preferred_element_type=jnp.float32,
    )
    finished = finished.astype(jnp.bfloat16)
    tok_rows = finished.shape[0]
    blocks = lax.axis_size("dp")
    share = local_cols.shape[1]
    sectioned = finished.reshape(tok_rows, blocks, 1, share)
    placed = lax.all_to_all(sectioned, "mp", split_axis=1, concat_axis=2, tiled=True)
    return placed.reshape(tok_rows, placed.shape[1] * placed.shape[2] * share)


def kernel(nz, a_ref, w_ref, o_ref, big, acts, outs, send_sem, recv_sem, act_send, act_recv, loc_sem, act_loc, out_sem):
    d, x = lax.axis_index("dp"), lax.axis_index("mp")
    z, y, c = d // 4, (d // 2) % 2, d % 2
    half = nz // 2
    width, depth = w_ref.shape
    rows = a_ref.shape[0]
    steps = width // UNIT
    first_dup = steps - DUP
    per, mid = LANES // UNIT, width // LANES
    loose = (width - mid * LANES) // UNIT
    lag = SKEW * (nz + 2)
    core_dev = (d + 1 - 2 * c, x)
    y_dev = (d + 2 - 4 * y, x)
    x_dev = (d, 1 - x)
    up_dev = (lax.rem(d + 4, 4 * nz), x)
    down_dev = (lax.rem(d + 4 * nz - 4, 4 * nz), x)
    can_up, can_down, never = z < nz - 1, z > 0, z < 0

    def unit_of(cc, t):
        return lax.rem(t + (steps - loose) * (1 - cc), steps)

    def part(zz, yy, xx, cc, t):
        row = pl.multiple_of(cc * width + unit_of(cc, t) * UNIT, UNIT)
        return big.at[zz * 2 + yy, xx, pl.ds(row, UNIT), :]

    def own_copy(t):
        row = pl.multiple_of(unit_of(c, t) * UNIT, UNIT)
        return pltpu.make_async_copy(w_ref.at[pl.ds(row, UNIT), :], part(z, y, x, c, t), loc_sem.at[t])

    own_act = pltpu.make_async_copy(
        a_ref, acts.at[:, pl.ds(pl.multiple_of(x * depth, LANES), depth)], act_loc.at[0])

    def begin(t, carry):
        own_copy(t).start()
        return carry

    lax.fori_loop(0, steps, begin, 0)
    own_act.start()

    barrier = pltpu.get_barrier_semaphore()
    for dev in (core_dev, y_dev, x_dev):
        pl.semaphore_signal(barrier, inc=1, device_id=dev, device_id_type=MESH)

    @pl.when(can_up)
    def _():
        pl.semaphore_signal(barrier, inc=1, device_id=up_dev, device_id_type=MESH)

    @pl.when(can_down)
    def _():
        pl.semaphore_signal(barrier, inc=1, device_id=down_dev, device_id_type=MESH)

    pl.semaphore_wait(barrier, 3 + can_up.astype(jnp.int32) + can_down.astype(jnp.int32))

    def copy(kind, zz, yy, xx, cc, t, dev):
        piece = part(zz, yy, xx, cc, t)
        return pltpu.make_async_remote_copy(
            src_ref=piece, dst_ref=piece, send_sem=send_sem.at[kind, zz, t],
            recv_sem=recv_sem.at[zz, yy, xx * 2 + cc, t], device_id=dev, device_id_type=MESH)

    def along(kind, zz, yy, t, up, down, act):
        @pl.when(up)
        def _():
            act(copy(kind, zz, yy, x, c, t, up_dev))

        @pl.when(down)
        def _():
            act(copy(kind + 1, zz, yy, x, c, t, down_dev))

    def lane_piece(zz, t, up, down, own, act):
        along(0, zz, y, t, up, down, act)
        mine = zz // half == x
        over_y = (t < first_dup) | (t < steps if own else never)

        @pl.when(mine & over_y)
        def _():
            act(copy(2, zz, y, x, c, t, y_dev))

        @pl.when(mine)
        def _():
            act(copy(3, zz, y, x, c, t, core_dev))

        @pl.when(~mine)
        def _():
            act(copy(2, zz, y, x, c, t, x_dev))

        if own:
            @pl.when(~mine & (t >= first_dup))
            def _():
                act(copy(3, zz, y, x, c, t, y_dev))

    def twin_piece(zz, t, up, down, act):
        along(8, zz, 1 - y, t, up, down, act)

        @pl.when(zz // half == x)
        def _():
            act(copy(6, zz, 1 - y, x, c, t, core_dev))

        @pl.when(zz // half != x)
        def _():
            act(copy(6, zz, 1 - y, x, c, t, x_dev))

    def own_stage(t, act, arrive):
        lane_piece(z, t, can_up, can_down, True, act)

    def z_stage(dist, t, act, arrive):
        @pl.when(z >= dist)
        def _():
            arrive(z - dist, y, x, c, t)
            lane_piece(z - dist, t, can_up, never, False, act)

        @pl.when(z + dist < nz)
        def _():
            arrive(z + dist, y, x, c, t)
            lane_piece(z + dist, t, never, can_down, False, act)

    def twin_own_stage(t, act, arrive):
        arrive(z, 1 - y, x, c, t)
        twin_piece(z, t, can_up, can_down, act)

    def twin_z_stage(dist, t, act, arrive):
        @pl.when(z >= dist)
        def _():
            arrive(z - dist, 1 - y, x, c, t)
            twin_piece(z - dist, t, can_up, never, act)

        @pl.when(z + dist < nz)
        def _():
            arrive(z + dist, 1 - y, x, c, t)
            twin_piece(z + dist, t, never, can_down, act)

    def x_stage(h, t, act, arrive):
        zz = x * half + h
        arrive(zz, y, 1 - x, c, t)

        @pl.when(t < first_dup)
        def _():
            act(copy(4, zz, y, 1 - x, c, t, y_dev))

        act(copy(5, zz, y, 1 - x, c, t, core_dev))

    def twin_x_stage(h, t, act, arrive):
        zz = x * half + h
        arrive(zz, 1 - y, 1 - x, c, t)
        act(copy(7, zz, 1 - y, 1 - x, c, t, core_dev))

    def y_stage(h, other, t, act, arrive):
        zz = x * half + h
        xx = 1 - x if other else x
        arrive(zz, 1 - y, xx, c, t)
        act(copy(6 + other, zz, 1 - y, xx, c, t, core_dev))

    def start(cp):
        cp.start()

    def drain(cp):
        cp.wait_send()

    def arrive(zz, yy, xx, cc, t):
        copy(0, zz, yy, xx, cc, t, core_dev).wait_recv()

    def no_arrive(zz, yy, xx, cc, t):
        pass

    act_rows = rows // ACT_PIECES

    def act_copy(k, xx):
        piece = pl.ds(pl.multiple_of(k * act_rows, 16), act_rows)
        return pltpu.make_async_remote_copy(
            src_ref=a_ref.at[piece, :],
            dst_ref=acts.at[piece, pl.ds(pl.multiple_of(xx * depth, LANES), depth)],
            send_sem=act_send.at[k], recv_sem=act_recv.at[k],
            device_id=x_dev, device_id_type=MESH)

    def out_copy(b, g):
        cols = pl.ds(pl.multiple_of(b * 2 * width + g * LANES, LANES), LANES)
        return pltpu.make_async_copy(outs.at[:, cols], o_ref.at[:, cols], out_sem.at[b, g])

    def multiply(g):
        cols = pl.ds(pl.multiple_of(g * LANES, LANES), LANES)
        for b in range(0, 2 * half, 2):
            base = x * 2 * half + b
            rhs = jnp.concatenate([
                jnp.concatenate([big[base + k, 0, cols, :], big[base + k, 1, cols, :]], axis=1)
                for k in range(2)
            ], axis=0)
            res = lax.dot_general(
                acts[...], rhs, (((1,), (1,)), ((), ())), preferred_element_type=jnp.float32
            ).astype(jnp.bfloat16)
            for k in range(2):
                at = pl.ds(pl.multiple_of((b + k) * 2 * width + g * LANES, LANES), LANES)
                outs[:, at] = res[:, k * LANES:(k + 1) * LANES]
                out_copy(b + k, g).start()

    def product(t):
        for h in range(half):
            for yy in range(2):
                for xx in range(2):
                    arrive(x * half + h, yy, xx, 1 - c, t)
        past = t - (loose - 1)
        k = past // per

        def one(j, carry):
            multiply(jnp.where(past == 0, mid, jnp.where(j == 0, k - 1, mid + k)))
            return carry

        @pl.when((past >= 0) & (lax.rem(past + per, per) == 0))
        def _():
            lax.fori_loop(0, jnp.where(past == 0, 1, 2), one, 0)

    def step(i, carry):
        def at(t, stage, low=0, high=steps):
            pl.when((t >= low) & (t < high))(functools.partial(stage, t))

        def go(stage, *lead):
            return lambda t: stage(*lead, t, start, arrive)

        def own(t):
            own_copy(t).wait()
            own_stage(t, start, arrive)

        at(i, own)
        for dist in range(1, nz):
            at(i - SKEW * dist, go(z_stage, dist))

        @pl.when((i >= 1) & (i <= ACT_PIECES))
        def _():
            act_copy(i - 1, x).start()

        @pl.when(i == lag)
        def _():
            own_act.wait()
            for k in range(ACT_PIECES):
                act_copy(k, 1 - x).wait_recv()

        at(i - lag, product)
        for h in range(half):
            away = jnp.abs(z - (x * half + h))
            at(i - SKEW * (away + 1), go(x_stage, h))
            at(i - SKEW * (away + 2), go(twin_x_stage, h), first_dup)
            at(i - SKEW * (away + 1), go(y_stage, h, 0), 0, first_dup)
            at(i - SKEW * (away + 2), go(y_stage, h, 1), 0, first_dup)
        at(i - SKEW, go(twin_own_stage), first_dup)
        for dist in range(1, nz):
            at(i - SKEW * (1 + dist), go(twin_z_stage, dist), first_dup)
        return carry

    lax.fori_loop(0, steps + lag, step, 0)

    def finish(t, carry):
        own_stage(t, drain, no_arrive)
        for dist in range(1, nz):
            z_stage(dist, t, drain, no_arrive)
        for h in range(half):
            x_stage(h, t, drain, no_arrive)

        @pl.when(t < first_dup)
        def _():
            for h in range(half):
                y_stage(h, 0, t, drain, no_arrive)
                y_stage(h, 1, t, drain, no_arrive)

        @pl.when(t >= first_dup)
        def _():
            twin_own_stage(t, drain, no_arrive)
            for dist in range(1, nz):
                twin_z_stage(dist, t, drain, no_arrive)
            for h in range(half):
                twin_x_stage(h, t, drain, no_arrive)

        return carry

    lax.fori_loop(0, steps, finish, 0)
    for k in range(ACT_PIECES):
        act_copy(k, x).wait_send()
    for b in range(2 * half):
        for g in range(2 * width // LANES):
            out_copy(b, g).wait()


def gathered(nz, activations, projection):
    rows, depth = activations.shape
    width = projection.shape[1]
    steps, groups, half = width // UNIT, 2 * width // LANES, nz // 2
    columns = nz * 2 * width
    dma = pltpu.SemaphoreType.DMA
    return pl.pallas_call(
        functools.partial(kernel, nz),
        out_shape=jax.ShapeDtypeStruct((rows, columns), jnp.bfloat16),
        in_specs=[pl.BlockSpec(memory_space=pl.ANY)] * 2,
        out_specs=pl.BlockSpec(memory_space=pl.ANY),
        scratch_shapes=[
            pltpu.VMEM((nz * 2, 2, 2 * width, depth), jnp.bfloat16),
            pltpu.VMEM((rows, 2 * depth), jnp.bfloat16),
            pltpu.VMEM((rows, columns), jnp.bfloat16),
            dma((10, nz, steps)),
            dma((nz, 2, 4, steps)),
            dma((ACT_PIECES,)),
            dma((ACT_PIECES,)),
            dma((steps,)),
            dma((1,)),
            dma((2 * half, groups)),
        ],
        compiler_params=pltpu.CompilerParams(
            collective_id=0, has_side_effects=True, vmem_limit_bytes=60 * 2**20),
    )(activations, projection.T)


def solution(mesh):
    n_dp, n_mp = mesh.shape["dp"], mesh.shape["mp"]

    def shards(activations, projection):
        rows, depth = activations.shape
        width = projection.shape[1]
        nz = n_dp // 4
        fits = (
            n_mp == 2 and n_dp % 8 == 0 and width % LANES == LANES // 2
            and width > LANES and depth % LANES == 0 and rows % (16 * ACT_PIECES) == 0
            and nz * 2 * 2 * depth * 2 * width * 2 <= 36 * 2**20 and nz <= 4
        )
        if fits:
            return gathered(nz, activations, projection)
        return general(activations, projection)

    placed = (P("dp", "mp"), P("mp", "dp"))
    return jax.shard_map(
        shards, mesh=mesh, in_specs=placed, out_specs=P("dp", "mp"), check_vma=False
    )
```
